32 devices in a mesh: vocab: 8 (over z, y), batch: 4 (over x, core).
Axes of the slice: x: 2, y: 2, z: 4, core: 2. Of those that a mesh axis runs over, the one named last changes fastest.
Arguments:
- latent_state_rows: bfloat16 [64, 8192], P('batch', 'vocab'), may hold values from -90 to 90
- closing_rescale_coeffs: bfloat16 [8192], replicated, may hold values from 0.5 to 1.5
- output_projection_matrix: bfloat16 [8192, 131072], P(None, ('vocab', 'batch')), may hold values from -3.7565048 to 3.7565048
- config_heat_values: float32 [16], replicated, may hold values from 0.7 to 1.4
- sequence_config_choice: int32 [64], replicated, may hold values from 0 to 15
- ranked_choice_ids: int32 [64, 128], replicated, may hold values from 0 to 131071
- keep_count: int32 [64], replicated, may hold values from 2 to 128
Outputs:
- log_norm: float32 [64], P('batch')
- kept_mass: float32 [64], P('batch')
- renormed: float32 [64, 128], P('batch')
The draws below stay inside these ranges and needn't reach their ends.
All inputs are finite; a program needn't handle non-finite values.
Results may differ from the reference program's by a relative error of at most 0.0048.
Values may be sent and summed in bfloat16 or wider, within the bound.
A program may use at most 128 MiB of HBM per device.

```python
import math
import jax
import jax.numpy as jnp
from jax import lax

D = 8192
VOCAB = 131072
CAND = 128
SAMPLER_CONFIGS = 16
SG = 16
SLOTS = 64
N_VOCAB = 8
N_BATCH = 4


def weight_block(key, block):
    return jnp.clip(jax.random.normal(jax.random.fold_in(jax.random.fold_in(key, 11), block), (D, 128), jnp.float32), -5.0, 5.0)


def column_scale(key):
    position = jnp.arange(VOCAB, dtype=jnp.float32) / VOCAB
    spread = jnp.exp(jax.random.uniform(jax.random.fold_in(key, 12), (VOCAB,), jnp.float32, math.log(0.45), math.log(2.2)))
    trend = 0.75 + 0.5 * position
    return 2.0 * spread * trend


def drawn_pairs():
    pairs = []
    targets = [160.0, 200.0, 240.0, 160.0, 200.0, 240.0]
    for number in range(6):
        first_id = (5003 + 24011 * number) % VOCAB
        second_id = (first_id + 7) % VOCAB
        row_index = number * SLOTS // 6
        pairs.append((first_id, second_id, row_index, targets[number]))
    return pairs


def draw_output_projection_matrix(key, part):
    blocks = jax.vmap(lambda block: weight_block(key, block), out_axes=1)(jnp.arange(VOCAB // 128))
    matrix = blocks.reshape(D, VOCAB) * (column_scale(key) / math.sqrt(D))[None, :]
    return matrix.astype(jnp.bfloat16)


def draw_latent_state_rows(key, part):
    values = jnp.clip(jax.random.normal(jax.random.fold_in(key, 13), (SLOTS, D), jnp.float32), -5.0, 5.0)
    return values.astype(jnp.bfloat16)


def draw_ranked_choice_ids(key, part):
    ids = jax.random.randint(jax.random.fold_in(key, 16), (SLOTS, CAND), 0, VOCAB, jnp.int32)
    shard_count = N_VOCAB * N_BATCH
    shard_width = VOCAB // shard_count
    group_of = jnp.arange(SLOTS, dtype=jnp.int32) // SG
    offsets = jax.random.randint(jax.random.fold_in(key, 17), (SLOTS, 2), 0, shard_width, jnp.int32)
    near_shard = (group_of + 1) % shard_count
    far_shard = (group_of + shard_count // 2) % shard_count
    ids = ids.at[:, 0].set(near_shard * shard_width + offsets[:, 0])
    ids = ids.at[:, 1].set(far_shard * shard_width + offsets[:, 1])
    for first_id, second_id, row_index, target in drawn_pairs():
        ids = ids.at[row_index, 0].set(jnp.int32(first_id))
        ids = ids.at[row_index, 1].set(jnp.int32(second_id))
    return ids


def touch_ends(values, own_key, low, top_value):
    extent = values.shape
    place = [jax.random.randint(jax.random.fold_in(own_key, axis), (), 0, extent[axis]) for axis in range(len(extent))]
    values = values.at[tuple(place)].set(low)
    longest = extent.index(max(extent))
    place[longest] = (place[longest] + 1) % extent[longest]
    return values.at[tuple(place)].set(top_value)


def setup_inputs(seed: int = 0) -> dict:
    key_list = jax.random.split(jax.random.key(seed), 8)
    latent_state_rows = draw_latent_state_rows(jax.random.fold_in(key_list[7], 71), 0)
    closing_rescale_coeffs = jnp.clip(1.0 + 0.1 * jax.random.normal(key_list[1], (D,), jnp.float32), 0.5, 1.5).astype(jnp.bfloat16)
    output_projection_matrix = draw_output_projection_matrix(jax.random.fold_in(key_list[7], 71), 0)
    config_heat_values = jnp.clip(jnp.exp(jax.random.uniform(key_list[3], (SAMPLER_CONFIGS,), jnp.float32, math.log(0.7), math.log(1.4))), 0.7, 1.4)
    sequence_config_choice = touch_ends(jax.random.randint(key_list[4], (SLOTS,), 0, SAMPLER_CONFIGS), jax.random.fold_in(key_list[4], 1), 0, SAMPLER_CONFIGS - 1).astype(jnp.int32)
    ranked_choice_ids = draw_ranked_choice_ids(jax.random.fold_in(key_list[7], 71), 0)
    keep_count = touch_ends(jax.random.randint(key_list[6], (SLOTS,), 2, CAND + 1), jax.random.fold_in(key_list[6], 1), 2, CAND).astype(jnp.int32)
    return {"latent_state_rows": latent_state_rows, "closing_rescale_coeffs": closing_rescale_coeffs, "output_projection_matrix": output_projection_matrix, "config_heat_values": config_heat_values, "sequence_config_choice": sequence_config_choice, "ranked_choice_ids": ranked_choice_ids, "keep_count": keep_count}


epsilon = 1e-06

def reference(latent_state_rows, closing_rescale_coeffs, output_projection_matrix, config_heat_values, sequence_config_choice, ranked_choice_ids, keep_count):
    values = latent_state_rows.astype(jnp.float32)
    mean_square = lax.optimization_barrier(jnp.mean(values * values, axis=1, keepdims=True))
    normed = (values * lax.rsqrt(mean_square + epsilon) * closing_rescale_coeffs.astype(jnp.float32)[None, :]).astype(jnp.bfloat16)
    unnormalized_scores = jnp.dot(normed, output_projection_matrix, preferred_element_type=jnp.float32)
    config_membership = (sequence_config_choice[:, None] == jnp.arange(SAMPLER_CONFIGS, dtype=jnp.int32)[None, :]).astype(jnp.float32)
    sequence_heat_values = lax.optimization_barrier(jnp.sum(config_membership * config_heat_values[None, :], axis=1))
    divided_scores = unnormalized_scores / sequence_heat_values[:, None]
    row_top = lax.optimization_barrier(jnp.max(divided_scores, axis=1))
    row_total = lax.optimization_barrier(jnp.sum(jnp.exp(divided_scores - row_top[:, None]), axis=1))
    log_norm = row_top + jnp.log(row_total)
    picked = jnp.take_along_axis(divided_scores, ranked_choice_ids.astype(jnp.int32), axis=1)
    kept_mask = jnp.arange(CAND, dtype=jnp.int32)[None, :] < keep_count[:, None]
    kept_top = lax.optimization_barrier(jnp.max(jnp.where(kept_mask, picked, jnp.float32(-3e+38)), axis=1))
    shifted = jnp.where(kept_mask, picked - kept_top[:, None], jnp.float32(0.0))
    kept_exp = jnp.where(kept_mask, jnp.exp(shifted), jnp.float32(0.0))
    kept_sum = lax.optimization_barrier(jnp.sum(kept_exp, axis=1))
    kept_mass = kept_top + jnp.log(kept_sum) - log_norm
    return (log_norm, kept_mass, kept_exp / kept_sum[:, None])
```

```python
import functools

import jax
import jax.numpy as jnp
from jax import lax
from jax.experimental import pallas as pl
from jax.experimental.pallas import tpu as pltpu
from jax.sharding import PartitionSpec as P

MESH = pl.DeviceIdType.MESH
epsilon = 1e-06
LANES = 128
TILE = 256
STAT_ROWS = 8
BLOCK_COLS = 512
STREAM_BYTES = 48 * 1024 * 1024
LAST_ROWS = 512
LOW = -3e38


def iota(shape, axis):
    return lax.broadcasted_iota(jnp.int32, shape, axis)


def column_to_row(column):
    rows = column.shape[0]
    diagonal = iota((rows, LANES), 0) == iota((rows, LANES), 1)
    return jnp.sum(jnp.where(diagonal, column, 0.0), axis=0, keepdims=True)


def row_to_column(row, first, rows):
    width = row.shape[1]
    diagonal = iota((rows, width), 0) + first == iota((rows, width), 1)
    return jnp.sum(jnp.where(diagonal, row, 0.0), axis=1, keepdims=True)


def combine(parts, group):
    candidates = parts[0][:group, :]
    top = parts[0][group : group + 1, :]
    for part in parts[1:]:
        candidates = candidates + part[:group, :]
        top = jnp.maximum(top, part[group : group + 1, :])
    total = jnp.zeros_like(top)
    for part in parts:
        total = total + part[group + 1 : group + 2, :] * jnp.exp(
            part[group : group + 1, :] - top
        )
    return candidates, top, total


def flip(value, j):
    out = value
    bit = 1
    while bit <= j:
        if j & bit:
            out = out + bit * (1 - 2 * ((value // bit) % 2))
        bit *= 2
    return out


def kernel(n_v, n_b, n_early, specs, *refs):
    pl.run_scoped(lambda *accs: program(n_v, n_b, n_early, accs, *refs), *specs)


def program(
    n_v,
    n_b,
    n_early,
    accs,
    x_hbm,
    gain_hbm,
    w_hbm,
    heat_hbm,
    choice_hbm,
    ids_hbm,
    keep_hbm,
    out_ref,
    wbuf,
    xbuf,
    lhs,
    gain_in,
    gain_row,
    heat_ref,
    choice_ref,
    ids_ref,
    keep_ref,
    z_stat,
    p_stat,
    stat_out,
    outbox,
    inbox,
    midbox,
    lastbox,
    w_sem,
    l_sem,
    in_sem,
    x_recv,
    x_send,
    z_recv,
    z_send,
    p_recv,
    p_send,
    t_recv,
    t_send,
    u_recv,
    u_send,
):
    v = lax.axis_index("vocab")
    b = lax.axis_index("batch")
    side = n_b // 2
    n_z = n_v // side
    z = v // side
    y = v % side
    x = b // 2
    c = b % 2
    n_p = 2 * side * side
    group, fpd = x_hbm.shape
    slots = n_b * group
    depth, cols = w_hbm.shape
    n_slots, kz, bc = wbuf.shape
    n_blocks = cols // bc
    halves = bc // TILE
    n_last = max(1, kz // LAST_ROWS)

    def device(x_, y_, z_, c_):
        return (z_ * side + y_, 2 * x_ + c_)

    def place(x_, y_, c_):
        return (x_ * side + y_) * 2 + c_

    mine = place(x, y, c)

    plane = []
    for dx in range(side):
        for dy in range(side):
            for dc in range(2):
                if dx + dy + dc > 0:
                    plane.append(((x + dx) % side, (y + dy) % side, (c + dc) % 2))
    order = [flip(z, j) for j in range(n_z)]

    loads = [
        pltpu.make_async_copy(src, dst, in_sem.at[i])
        for i, (src, dst) in enumerate(
            [
                (x_hbm, xbuf.at[v, b]),
                (gain_hbm, gain_in),
                (heat_hbm, heat_ref),
                (choice_hbm, choice_ref),
                (ids_hbm, ids_ref),
                (keep_hbm, keep_ref),
            ]
        )
    ]
    for copy in loads:
        copy.start()

    tasks = [(j, n) for j in range(n_z) for n in range(n_early)]
    tasks += [(j, n) for n in range(n_early, n_blocks) for j in range(n_z)]
    n_tasks = len(tasks)

    def stream(t):
        j, n = tasks[t]
        slot = t % n_slots
        row = pl.multiple_of(order[j] * kz, kz)
        columns = pl.ds(n * bc, bc)
        if t < n_tasks - 1:
            return [
                pltpu.make_async_copy(
                    w_hbm.at[pl.ds(row, kz), columns], wbuf.at[slot], w_sem.at[slot]
                )
            ]
        piece = kz // n_last
        return [
            pltpu.make_async_copy(
                w_hbm.at[pl.ds(row + i * piece, piece), columns],
                wbuf.at[slot, pl.ds(i * piece, piece)],
                l_sem.at[i],
            )
            for i in range(n_last)
        ]

    for t in range(min(n_slots, n_tasks)):
        for copy in stream(t):
            copy.start()

    barrier = pltpu.get_barrier_semaphore()
    for j in range(1, n_z):
        pl.semaphore_signal(
            barrier, inc=1, device_id=device(x, y, order[j], c), device_id_type=MESH
        )
    for px, py, pc in plane:
        pl.semaphore_signal(
            barrier, inc=1, device_id=device(px, py, z, pc), device_id_type=MESH
        )

    loads[0].wait()
    own = xbuf[v, b].astype(jnp.float32)
    own = own * own
    partial = own[:, :LANES]
    for t in range(1, fpd // LANES):
        partial = partial + own[:, t * LANES : (t + 1) * LANES]
    partial = column_to_row(jnp.sum(partial, axis=1, keepdims=True))
    stat_out[0] = partial
    z_stat[z] = partial

    pl.semaphore_wait(barrier, n_z - 1 + n_p - 1)

    sent = []

    def send(src, dst, send_sem, recv_sem, to):
        copy = pltpu.make_async_remote_copy(
            src_ref=src,
            dst_ref=dst,
            send_sem=send_sem,
            recv_sem=recv_sem,
            device_id=to,
            device_id_type=MESH,
        )
        copy.start()
        sent.append(copy)

    counter = [0]

    def forward(v_, b_, to):
        block = xbuf.at[v_, b_]
        send(block, block, x_send.at[counter[0]], x_recv.at[v_, b_], to)
        counter[0] += 1

    def arrived(v_, b_):
        pltpu.make_async_copy(x_hbm, xbuf.at[v_, b_], x_recv.at[v_, b_]).wait()

    def peers(i, first):
        a = 1 - c if first else c
        return (x + i * a) % side, (y + i * (1 - a)) % side

    def sources(i, first):
        a = 1 - c if first else c
        return (x + (side - i) * a) % side, (y + (side - i) * (1 - a)) % side

    for j in range(1, n_z):
        send(
            stat_out.at[0],
            z_stat.at[z],
            z_send.at[j],
            z_recv.at[z],
            device(x, y, order[j], c),
        )
    for j in reversed(range(1, n_z)):
        forward(v, b, device(x, y, order[j], c))

    def spread(v_, b_, first):
        if first:
            for i in range(1, side):
                px, py = peers(i, True)
                forward(v_, b_, device(px, py, z, c))
        for i in range(1, side):
            px, py = peers(i, False)
            forward(v_, b_, device(px, py, z, c))
        forward(v_, b_, device(x, y, z, 1 - c))

    def step_z(j):
        v_ = order[j] * side + y
        if j > 0:
            arrived(v_, b)
        spread(v_, b, True)

    def step_f(j):
        for i in range(1, side):
            fx, fy = sources(i, True)
            v_, b_ = order[j] * side + fy, 2 * fx + c
            arrived(v_, b_)
            spread(v_, b_, False)

    def step_s(j):
        for i in range(1, side):
            sx, sy = sources(i, False)
            v_, b_ = order[j] * side + sy, 2 * sx + c
            arrived(v_, b_)
            forward(v_, b_, device(x, y, z, 1 - c))

    def step_d(j):
        for i in range(1, side):
            for k in range(1, side):
                fx, fy = sources(i, True)
                sx, sy = sources(k, False)
                dx = (fx + sx - x + side) % side
                dy = (fy + sy - y + side) % side
                v_, b_ = order[j] * side + dy, 2 * dx + c
                arrived(v_, b_)
                forward(v_, b_, device(x, y, z, 1 - c))

    def stat_z():
        for j in range(1, n_z):
            source = order[j]
            pltpu.make_async_copy(
                stat_out.at[0], z_stat.at[source], z_recv.at[source]
            ).wait()
        total = z_stat[0]
        for j in range(1, n_z):
            total = total + z_stat[j]
        stat_out[1] = total
        p_stat[mine] = total
        for i, (px, py, pc) in enumerate(plane):
            send(
                stat_out.at[1],
                p_stat.at[mine],
                p_send.at[i],
                p_recv.at[mine],
                device(px, py, z, pc),
            )

    def stat_p():
        for px, py, pc in plane:
            source = place(px, py, pc)
            pltpu.make_async_copy(
                stat_out.at[1], p_stat.at[source], p_recv.at[source]
            ).wait()
        columns = []
        for bx in range(side):
            for bcore in range(2):
                total = p_stat[place(bx, 0, bcore)]
                for by in range(1, side):
                    total = total + p_stat[place(bx, by, bcore)]
                columns.append(row_to_column(total, 0, group))
        mean_square = jnp.concatenate(columns, axis=0) / depth
        return lax.rsqrt(mean_square + epsilon)

    step_z(0)
    done = {"z": 1, "f": 0, "s": 0, "d": 0}

    def advance(kind):
        if done[kind] < n_z:
            {"z": step_z, "f": step_f, "s": step_s, "d": step_d}[kind](done[kind])
            done[kind] += 1

    for copy in loads[1:]:
        copy.wait()
    gain_row[...] = gain_in[...].astype(jnp.float32)

    advance("f")
    advance("z")
    advance("s")
    advance("f")
    advance("z")
    advance("d")
    advance("s")
    stat_z()
    advance("f")
    advance("z")
    advance("d")
    advance("s")
    while done["z"] < n_z:
        advance("f")
        advance("z")
        advance("d")
        advance("s")
    factor = stat_p()

    choice = row_to_column(choice_ref[...].astype(jnp.float32), 0, slots)
    n_heat = heat_ref.shape[1]
    member = choice == iota((slots, n_heat), 1).astype(jnp.float32)
    heat = jnp.sum(jnp.where(member, heat_ref[...], 0.0), axis=1, keepdims=True)
    cool = 1.0 / heat

    local_ids = ids_ref[...] - (v * n_b + b) * cols
    tile_of = local_ids >> 7
    lane_of = local_ids & (LANES - 1)

    def normalise(j):
        for k in range(side):
            at = order[j] * side + k
            values = xbuf[at].reshape(slots, fpd).astype(jnp.float32)
            for t in range(fpd // LANES):
                lanes = slice(t * LANES, (t + 1) * LANES)
                gain = gain_row[pl.ds(at * (fpd // LANES) + t, 1), :]
                lhs[j, :, k * fpd + t * LANES : k * fpd + (t + 1) * LANES] = (
                    values[:, lanes] * factor * gain
                ).astype(jnp.bfloat16)

    def partner_blocks(j):
        for k in range(side):
            for bx in range(side):
                arrived(order[j] * side + k, 2 * bx + 1 - c)

    n_acc = len(accs) // halves
    for acc in accs:
        pltpu.matmul_pop(acc)
    state = [
        jnp.full((slots, LANES), LOW, jnp.float32),
        jnp.zeros((slots, LANES), jnp.float32),
        jnp.zeros((slots, LANES), jnp.float32),
    ]

    def run(t):
        j, n = tasks[t]
        slot = t % n_slots
        pieces = stream(t)
        rows = kz // len(pieces)
        at = (n % n_acc) * halves
        turn = 0
        for i, piece in enumerate(pieces):
            piece.wait()
            for k in range(rows // TILE):
                r = i * rows + k * TILE
                for q in range(halves):
                    pltpu.matmul_push_rhs(
                        wbuf[slot, r : r + TILE, q * TILE : (q + 1) * TILE],
                        staging_register=turn % 2,
                        mxu_index=q,
                    )
                    pltpu.matmul_acc_lhs(
                        accs[at + q],
                        lhs[j, :, r : r + TILE],
                        load_staged_rhs=turn % 2,
                    )
                turn += 1
        if t + n_slots < n_tasks:
            for copy in stream(t + n_slots):
                copy.start()

    def finish(n):
        top, total, picked = state
        at = (n % n_acc) * halves
        parts = []
        for q in range(halves):
            scores = pltpu.matmul_pop(accs[at + q]) * cool
            for h in range(TILE // LANES):
                parts.append(scores[:, h * LANES : (h + 1) * LANES])
        new_top = top
        for i, part in enumerate(parts):
            new_top = jnp.maximum(new_top, part)
            found = jnp.take_along_axis(
                part, lane_of, axis=1, mode="promise_in_bounds"
            )
            picked = jnp.where(tile_of == n * (bc // LANES) + i, found, picked)
        total = total * jnp.exp(top - new_top)
        for part in parts:
            total = total + jnp.exp(part - new_top)
        state[:] = [new_top, total, picked]

    pending = []
    t = 0
    for j in range(n_z):
        while done["d"] <= j:
            advance("f")
            advance("s")
            advance("d")
        partner_blocks(j)
        normalise(j)
        for n in range(n_early):
            run(t)
            t += 1
    pending = list(range(n_early))
    for n in range(n_early, n_blocks):
        while pending and (len(pending) >= n_acc or pending[0] % n_acc == n % n_acc):
            finish(pending.pop(0))
        for j in range(n_z):
            run(t)
            t += 1
            if pending:
                finish(pending.pop(0))
        pending.append(n)
    while pending:
        finish(pending.pop(0))

    top, total, picked = state
    peak = jnp.max(top, axis=1, keepdims=True)
    total = jnp.sum(total * jnp.exp(top - peak), axis=1, keepdims=True)
    for p in range(n_b):
        rows = slice(p * group, (p + 1) * group)
        outbox[p, :group, :] = picked[rows, :]
        outbox[p, group : group + 1, :] = column_to_row(peak[rows, :])
        outbox[p, group + 1 : group + 2, :] = column_to_row(total[rows, :])
        outbox[p, group + 2 :, :] = jnp.zeros((STAT_ROWS - 2, LANES), jnp.float32)

    for i, (px, py, pc) in enumerate(plane):
        send(
            outbox.at[2 * px + pc],
            inbox.at[mine],
            t_send.at[i],
            t_recv.at[mine],
            device(px, py, z, pc),
        )
    inbox[mine] = outbox[b]
    for px, py, pc in plane:
        source = place(px, py, pc)
        pltpu.make_async_copy(outbox.at[0], inbox.at[source], t_recv.at[source]).wait()
    candidates, top, total = combine([inbox[s] for s in range(n_p)], group)
    midbox[:group, :] = candidates
    midbox[group : group + 1, :] = top
    midbox[group + 1 : group + 2, :] = total
    midbox[group + 2 :, :] = jnp.zeros((STAT_ROWS - 2, LANES), jnp.float32)
    for j in range(1, n_z):
        send(midbox, lastbox.at[z], u_send.at[j], u_recv.at[z], device(x, y, order[j], c))
    lastbox[z] = midbox[...]
    for j in range(1, n_z):
        source = order[j]
        pltpu.make_async_copy(midbox, lastbox.at[source], u_recv.at[source]).wait()
    candidates, top, total = combine([lastbox[s] for s in range(n_z)], group)

    log_norm = top + jnp.log(jnp.where(total > 0.0, total, 1.0))
    cutoff = row_to_column(keep_ref[...].astype(jnp.float32), b * group, group)
    kept = iota((group, LANES), 1).astype(jnp.float32) < cutoff
    kept_top = jnp.max(jnp.where(kept, candidates, LOW), axis=1, keepdims=True)
    shifted = jnp.where(kept, candidates - kept_top, 0.0)
    kept_exp = jnp.where(kept, jnp.exp(shifted), 0.0)
    kept_sum = jnp.sum(kept_exp, axis=1, keepdims=True)
    kept_log = column_to_row(kept_top + jnp.log(kept_sum))
    out_ref[:group, :] = kept_exp / kept_sum
    out_ref[group : group + 1, :] = log_norm
    out_ref[group + 1 : group + 2, :] = kept_log - log_norm
    out_ref[group + 2 :, :] = jnp.zeros((STAT_ROWS - 2, LANES), jnp.float32)
    for copy in sent:
        copy.wait_send()


def split(all_ref, norm_ref, mass_ref, renorm_ref):
    group = renorm_ref.shape[0]
    renorm_ref[...] = all_ref[:group, :]
    norm_ref[...] = all_ref[group : group + 1, :group]
    mass_ref[...] = all_ref[group + 1 : group + 2, :group]


def solution(mesh):
    n_v, n_b = mesh.shape["vocab"], mesh.shape["batch"]

    def local(rows, gain, w, heat, choice, ids, keep):
        group, fpd = rows.shape
        depth, cols = w.shape
        slots = n_b * group
        side = n_b // 2
        n_z = n_v // side
        n_p = 2 * side * side
        kz = depth // n_z
        bc = min(cols, BLOCK_COLS)
        n_blocks = cols // bc
        n_early = max(1, n_blocks // 2)
        n_slots = min(n_z * n_blocks, max(2, STREAM_BYTES // (kz * bc * 2)))
        box = group + STAT_ROWS
        hops = side - 1
        n_sends = n_z - 1 + n_z * (4 * hops + 2 * hops * hops + 1)
        n_acc = max(n_early, min(2, n_blocks))
        accs = [
            pltpu.ACC(q)((slots, TILE), jnp.float32)
            for _ in range(n_acc)
            for q in range(bc // TILE)
        ]
        vmem = pl.BlockSpec(memory_space=pltpu.VMEM)
        anywhere = pl.BlockSpec(memory_space=pl.ANY)
        gain_rows = gain.reshape(depth // LANES, LANES)
        packed = pl.pallas_call(
            functools.partial(kernel, n_v, n_b, n_early, accs),
            out_shape=jax.ShapeDtypeStruct((box, LANES), jnp.float32),
            in_specs=[anywhere] * 7,
            out_specs=vmem,
            scratch_shapes=[
                pltpu.VMEM((n_slots, kz, bc), jnp.bfloat16),
                pltpu.VMEM((n_v, n_b, group, fpd), jnp.bfloat16),
                pltpu.VMEM((n_z, slots, kz), jnp.bfloat16),
                pltpu.VMEM(gain_rows.shape, jnp.bfloat16),
                pltpu.VMEM(gain_rows.shape, jnp.float32),
                pltpu.VMEM((1, heat.shape[0]), jnp.float32),
                pltpu.VMEM((1, slots), jnp.int32),
                pltpu.VMEM(ids.shape, jnp.int32),
                pltpu.VMEM((1, slots), jnp.int32),
                pltpu.VMEM((n_z, 1, LANES), jnp.float32),
                pltpu.VMEM((n_p, 1, LANES), jnp.float32),
                pltpu.VMEM((2, 1, LANES), jnp.float32),
                pltpu.VMEM((n_b, box, LANES), jnp.float32),
                pltpu.VMEM((n_p, box, LANES), jnp.float32),
                pltpu.VMEM((box, LANES), jnp.float32),
                pltpu.VMEM((n_z, box, LANES), jnp.float32),
                pltpu.SemaphoreType.DMA((n_slots,)),
                pltpu.SemaphoreType.DMA((max(1, kz // LAST_ROWS),)),
                pltpu.SemaphoreType.DMA((6,)),
                pltpu.SemaphoreType.DMA((n_v, n_b)),
                pltpu.SemaphoreType.DMA((n_sends,)),
                pltpu.SemaphoreType.DMA((n_z,)),
                pltpu.SemaphoreType.DMA((n_z,)),
                pltpu.SemaphoreType.DMA((n_p,)),
                pltpu.SemaphoreType.DMA((n_p,)),
                pltpu.SemaphoreType.DMA((n_p,)),
                pltpu.SemaphoreType.DMA((n_p,)),
                pltpu.SemaphoreType.DMA((n_z,)),
                pltpu.SemaphoreType.DMA((n_z,)),
            ],
            compiler_params=pltpu.CompilerParams(
                collective_id=0,
                has_side_effects=True,
                vmem_limit_bytes=60 * 1024 * 1024,
            ),
        )(
            rows,
            gain_rows,
            w,
            heat.reshape(1, -1),
            choice.reshape(1, -1),
            ids,
            keep.reshape(1, -1),
        )
        log_norm, mass, renormed = pl.pallas_call(
            split,
            out_shape=(
                jax.ShapeDtypeStruct((1, group), jnp.float32),
                jax.ShapeDtypeStruct((1, group), jnp.float32),
                jax.ShapeDtypeStruct((group, ids.shape[1]), jnp.float32),
            ),
            in_specs=[vmem],
            out_specs=(vmem, vmem, vmem),
        )(packed)
        return log_norm.reshape(group), mass.reshape(group), renormed

    placed = (P("batch", "vocab"), P(), P(None, ("vocab", "batch")), P(), P(), P(), P())
    return jax.shard_map(
        local,
        mesh=mesh,
        in_specs=placed,
        out_specs=(P("batch"), P("batch"), P("batch", None)),
        check_vma=False,
    )
```

```python
import functools

import jax
import jax.numpy as jnp
from jax import lax
from jax.experimental import pallas as pl
from jax.experimental.pallas import tpu as pltpu
from jax.sharding import PartitionSpec as P

MESH = pl.DeviceIdType.MESH
epsilon = 1e-06
LANES = 128
TILE = 256
STAT_ROWS = 2
BLOCK_COLS = 512
STREAM_BYTES = 48 * 1024 * 1024
LAST_ROWS = 512
LOW = -3e38


def iota(shape, axis):
    return lax.broadcasted_iota(jnp.int32, shape, axis)


def column_to_row(column):
    rows = column.shape[0]
    diagonal = iota((rows, LANES), 0) == iota((rows, LANES), 1)
    return jnp.sum(jnp.where(diagonal, column, 0.0), axis=0, keepdims=True)


def row_to_column(row, first, rows):
    width = row.shape[1]
    diagonal = iota((rows, width), 0) + first == iota((rows, width), 1)
    return jnp.sum(jnp.where(diagonal, row, 0.0), axis=1, keepdims=True)


def combine(parts, group):
    candidates = parts[0][:group, :]
    top = parts[0][group : group + 1, :]
    for part in parts[1:]:
        candidates = candidates + part[:group, :]
        top = jnp.maximum(top, part[group : group + 1, :])
    total = jnp.zeros_like(top)
    for part in parts:
        total = total + part[group + 1 : group + 2, :] * jnp.exp(
            part[group : group + 1, :] - top
        )
    return candidates, top, total


def flip(value, j):
    out = value
    bit = 1
    while bit <= j:
        if j & bit:
            out = out + bit * (1 - 2 * ((value // bit) % 2))
        bit *= 2
    return out


def kernel(n_v, n_b, n_early, specs, *refs):
    pl.run_scoped(lambda *accs: program(n_v, n_b, n_early, accs, *refs), *specs)


def program(
    n_v,
    n_b,
    n_early,
    accs,
    x_hbm,
    gain_hbm,
    w_hbm,
    heat_hbm,
    choice_hbm,
    ids_hbm,
    keep_hbm,
    out_ref,
    wbuf,
    xbuf,
    lhs,
    gain_in,
    gain_row,
    heat_ref,
    choice_ref,
    ids_ref,
    keep_ref,
    z_stat,
    p_stat,
    stat_out,
    outbox,
    inbox,
    midbox,
    lastbox,
    w_sem,
    l_sem,
    in_sem,
    x_recv,
    x_send,
    z_recv,
    z_send,
    p_recv,
    p_send,
    t_recv,
    t_send,
    u_recv,
    u_send,
):
    v = lax.axis_index("vocab")
    b = lax.axis_index("batch")
    side = n_b // 2
    n_z = n_v // side
    z = v // side
    y = v % side
    x = b // 2
    c = b % 2
    n_p = 2 * side * side
    group, fpd = x_hbm.shape
    slots = n_b * group
    depth, cols = w_hbm.shape
    n_slots, kz, bc = wbuf.shape
    n_blocks = cols // bc
    halves = bc // TILE
    n_last = max(1, kz // LAST_ROWS)

    def device(x_, y_, z_, c_):
        return (z_ * side + y_, 2 * x_ + c_)

    def place(x_, y_, c_):
        return (x_ * side + y_) * 2 + c_

    mine = place(x, y, c)

    plane = []
    for dx in range(side):
        for dy in range(side):
            for dc in range(2):
                if dx + dy + dc > 0:
                    plane.append(((x + dx) % side, (y + dy) % side, (c + dc) % 2))
    order = [flip(z, j) for j in range(n_z)]

    loads = [
        pltpu.make_async_copy(src, dst, in_sem.at[i])
        for i, (src, dst) in enumerate(
            [
                (x_hbm, xbuf.at[v, b]),
                (gain_hbm, gain_in),
                (heat_hbm, heat_ref),
                (choice_hbm, choice_ref),
                (ids_hbm, ids_ref),
                (keep_hbm, keep_ref),
            ]
        )
    ]
    for copy in loads:
        copy.start()

    tasks = [(j, n) for j in range(n_z) for n in range(n_early)]
    tasks += [(j, n) for n in range(n_early, n_blocks) for j in range(n_z)]
    n_tasks = len(tasks)

    def stream(t):
        j, n = tasks[t]
        slot = t % n_slots
        row = pl.multiple_of(order[j] * kz, kz)
        columns = pl.ds(n * bc, bc)
        if t < n_tasks - 1:
            return [
                pltpu.make_async_copy(
                    w_hbm.at[pl.ds(row, kz), columns], wbuf.at[slot], w_sem.at[slot]
                )
            ]
        piece = kz // n_last
        return [
            pltpu.make_async_copy(
                w_hbm.at[pl.ds(row + i * piece, piece), columns],
                wbuf.at[slot, pl.ds(i * piece, piece)],
                l_sem.at[i],
            )
            for i in range(n_last)
        ]

    for t in range(min(n_slots, n_tasks)):
        for copy in stream(t):
            copy.start(priority=1)

    barrier = pltpu.get_barrier_semaphore()
    for j in range(1, n_z):
        pl.semaphore_signal(
            barrier, inc=1, device_id=device(x, y, order[j], c), device_id_type=MESH
        )
    for px, py, pc in plane:
        pl.semaphore_signal(
            barrier, inc=1, device_id=device(px, py, z, pc), device_id_type=MESH
        )

    loads[0].wait()
    own = xbuf[v, b].astype(jnp.float32)
    own = own * own
    partial = own[:, :LANES]
    for t in range(1, fpd // LANES):
        partial = partial + own[:, t * LANES : (t + 1) * LANES]
    partial = column_to_row(jnp.sum(partial, axis=1, keepdims=True))
    stat_out[0] = partial
    z_stat[z] = partial

    pl.semaphore_wait(barrier, n_z - 1 + n_p - 1)

    sent = []

    def send(src, dst, send_sem, recv_sem, to):
        copy = pltpu.make_async_remote_copy(
            src_ref=src,
            dst_ref=dst,
            send_sem=send_sem,
            recv_sem=recv_sem,
            device_id=to,
            device_id_type=MESH,
        )
        copy.start()
        sent.append(copy)

    counter = [0]

    def forward(v_, b_, to):
        block = xbuf.at[v_, b_]
        send(block, block, x_send.at[counter[0]], x_recv.at[v_, b_], to)
        counter[0] += 1

    def arrived(v_, b_):
        pltpu.make_async_copy(x_hbm, xbuf.at[v_, b_], x_recv.at[v_, b_]).wait()

    same = [(dx, dy) for dx in range(side) for dy in range(side) if dx + dy > 0]
    same.sort(key=lambda d: -d[0] - d[1])

    for j in range(1, n_z):
        send(
            stat_out.at[0],
            z_stat.at[z],
            z_send.at[j],
            z_recv.at[z],
            device(x, y, order[j], c),
        )
    for j in reversed(range(1, n_z)):
        forward(v, b, device(x, y, order[j], c))

    def step_z(j):
        v_ = order[j] * side + y
        if j > 0:
            arrived(v_, b)
        for dx, dy in same:
            forward(v_, b, device((x + dx) % side, (y + dy) % side, z, c))
        forward(v_, b, device(x, y, z, 1 - c))

    def step_p(j):
        for dx, dy in reversed(same):
            px, py = (x - dx + side) % side, (y - dy + side) % side
            v_, b_ = order[j] * side + py, 2 * px + c
            arrived(v_, b_)
            forward(v_, b_, device(x, y, z, 1 - c))

    def stat_z():
        for j in range(1, n_z):
            source = order[j]
            pltpu.make_async_copy(
                stat_out.at[0], z_stat.at[source], z_recv.at[source]
            ).wait()
        total = z_stat[0]
        for j in range(1, n_z):
            total = total + z_stat[j]
        stat_out[1] = total
        p_stat[mine] = total
        for i, (px, py, pc) in enumerate(plane):
            send(
                stat_out.at[1],
                p_stat.at[mine],
                p_send.at[i],
                p_recv.at[mine],
                device(px, py, z, pc),
            )

    def stat_p():
        for px, py, pc in plane:
            source = place(px, py, pc)
            pltpu.make_async_copy(
                stat_out.at[1], p_stat.at[source], p_recv.at[source]
            ).wait()
        columns = []
        for bx in range(side):
            for bcore in range(2):
                total = p_stat[place(bx, 0, bcore)]
                for by in range(1, side):
                    total = total + p_stat[place(bx, by, bcore)]
                columns.append(row_to_column(total, 0, group))
        mean_square = jnp.concatenate(columns, axis=0) / depth
        return lax.rsqrt(mean_square + epsilon)

    step_z(0)
    for copy in loads[1:]:
        copy.wait()
    gain_row[...] = gain_in[...].astype(jnp.float32)
    early = max(1, n_z // 2)
    for j in range(1, early):
        step_z(j)
    step_p(0)
    for j in range(early, n_z - 1):
        step_z(j)
    stat_z()
    step_z(n_z - 1)
    for j in range(1, early):
        step_p(j)
    factor = stat_p()

    choice = row_to_column(choice_ref[...].astype(jnp.float32), 0, slots)
    n_heat = heat_ref.shape[1]
    member = choice == iota((slots, n_heat), 1).astype(jnp.float32)
    heat = jnp.sum(jnp.where(member, heat_ref[...], 0.0), axis=1, keepdims=True)
    cool = 1.0 / heat

    local_ids = ids_ref[...] - (v * n_b + b) * cols
    tile_of = local_ids >> 7
    lane_of = local_ids & (LANES - 1)

    def normalise(j):
        for k in range(side):
            at = order[j] * side + k
            values = xbuf[at].reshape(slots, fpd).astype(jnp.float32)
            for t in range(fpd // LANES):
                lanes = slice(t * LANES, (t + 1) * LANES)
                gain = gain_row[pl.ds(at * (fpd // LANES) + t, 1), :]
                lhs[j, :, k * fpd + t * LANES : k * fpd + (t + 1) * LANES] = (
                    values[:, lanes] * factor * gain
                ).astype(jnp.bfloat16)

    def partner_blocks(j):
        for k in range(side):
            for bx in range(side):
                arrived(order[j] * side + k, 2 * bx + 1 - c)

    n_acc = len(accs) // halves
    for acc in accs:
        pltpu.matmul_pop(acc)
    state = [
        jnp.full((slots, LANES), LOW, jnp.float32),
        jnp.zeros((slots, LANES), jnp.float32),
        jnp.zeros((slots, LANES), jnp.float32),
    ]

    def run(t):
        j, n = tasks[t]
        slot = t % n_slots
        pieces = stream(t)
        rows = kz // len(pieces)
        at = (n % n_acc) * halves
        turn = 0
        for i, piece in enumerate(pieces):
            piece.wait()
            for k in range(rows // TILE):
                r = i * rows + k * TILE
                for q in range(halves):
                    pltpu.matmul_push_rhs(
                        wbuf[slot, r : r + TILE, q * TILE : (q + 1) * TILE],
                        staging_register=turn % 2,
                        mxu_index=q,
                    )
                    pltpu.matmul_acc_lhs(
                        accs[at + q],
                        lhs[j, :, r : r + TILE],
                        load_staged_rhs=turn % 2,
                    )
                turn += 1
        if t + n_slots < n_tasks:
            for copy in stream(t + n_slots):
                copy.start(priority=1)

    def finish(n):
        top, total, picked = state
        at = (n % n_acc) * halves
        parts = []
        for q in range(halves):
            scores = pltpu.matmul_pop(accs[at + q]) * cool
            for h in range(TILE // LANES):
                parts.append(scores[:, h * LANES : (h + 1) * LANES])
        new_top = top
        for i, part in enumerate(parts):
            new_top = jnp.maximum(new_top, part)
            found = jnp.take_along_axis(
                part, lane_of, axis=1, mode="promise_in_bounds"
            )
            picked = jnp.where(tile_of == n * (bc // LANES) + i, found, picked)
        total = total * jnp.exp(top - new_top)
        for part in parts:
            total = total + jnp.exp(part - new_top)
        state[:] = [new_top, total, picked]

    pending = []
    t = 0
    for j in range(n_z):
        partner_blocks(j)
        if early <= j + early - 1 < n_z and j > 0:
            step_p(j + early - 1)
        normalise(j)
        for n in range(n_early):
            run(t)
            t += 1
    pending = list(range(n_early))
    for n in range(n_early, n_blocks):
        while pending and (len(pending) >= n_acc or pending[0] % n_acc == n % n_acc):
            finish(pending.pop(0))
        for j in range(n_z):
            run(t)
            t += 1
            if pending:
                finish(pending.pop(0))
        pending.append(n)
    while pending:
        finish(pending.pop(0))

    top, total, picked = state
    peak = jnp.max(top, axis=1, keepdims=True)
    total = jnp.sum(total * jnp.exp(top - peak), axis=1, keepdims=True)
    for p in range(n_b):
        rows = slice(p * group, (p + 1) * group)
        outbox[p, :group, :] = picked[rows, :]
        outbox[p, group : group + 1, :] = column_to_row(peak[rows, :])
        outbox[p, group + 1 : group + 2, :] = column_to_row(total[rows, :])

    for i, (px, py, pc) in enumerate(plane):
        send(
            outbox.at[2 * px + pc],
            inbox.at[mine],
            t_send.at[i],
            t_recv.at[mine],
            device(px, py, z, pc),
        )
    inbox[mine] = outbox[b]
    for px, py, pc in plane:
        source = place(px, py, pc)
        pltpu.make_async_copy(outbox.at[0], inbox.at[source], t_recv.at[source]).wait()
    candidates, top, total = combine([inbox[s] for s in range(n_p)], group)
    midbox[:group, :] = candidates
    midbox[group : group + 1, :] = top
    midbox[group + 1 : group + 2, :] = total
    for j in range(1, n_z):
        send(midbox, lastbox.at[z], u_send.at[j], u_recv.at[z], device(x, y, order[j], c))
    lastbox[z] = midbox[...]
    for j in range(1, n_z):
        source = order[j]
        pltpu.make_async_copy(midbox, lastbox.at[source], u_recv.at[source]).wait()
    candidates, top, total = combine([lastbox[s] for s in range(n_z)], group)

    log_norm = top + jnp.log(jnp.where(total > 0.0, total, 1.0))
    cutoff = row_to_column(keep_ref[...].astype(jnp.float32), b * group, group)
    kept = iota((group, LANES), 1).astype(jnp.float32) < cutoff
    kept_top = jnp.max(jnp.where(kept, candidates, LOW), axis=1, keepdims=True)
    shifted = jnp.where(kept, candidates - kept_top, 0.0)
    kept_exp = jnp.where(kept, jnp.exp(shifted), 0.0)
    kept_sum = jnp.sum(kept_exp, axis=1, keepdims=True)
    kept_log = column_to_row(kept_top + jnp.log(kept_sum))
    out_ref[:group, :] = kept_exp / kept_sum
    out_ref[group : group + 1, :] = log_norm
    out_ref[group + 1 : group + 2, :] = kept_log - log_norm
    for copy in sent:
        copy.wait_send()


def split(all_ref, norm_ref, mass_ref, renorm_ref):
    group = renorm_ref.shape[0]
    renorm_ref[...] = all_ref[:group, :]
    norm_ref[...] = all_ref[group : group + 1, :group]
    mass_ref[...] = all_ref[group + 1 : group + 2, :group]


def solution(mesh):
    n_v, n_b = mesh.shape["vocab"], mesh.shape["batch"]

    def local(rows, gain, w, heat, choice, ids, keep):
        group, fpd = rows.shape
        depth, cols = w.shape
        slots = n_b * group
        side = n_b // 2
        n_z = n_v // side
        n_p = 2 * side * side
        kz = depth // n_z
        bc = min(cols, BLOCK_COLS)
        n_blocks = cols // bc
        n_early = max(1, n_blocks - n_blocks // 4)
        n_slots = min(n_z * n_blocks, max(2, STREAM_BYTES // (kz * bc * 2)))
        box = group + STAT_ROWS
        n_sends = n_z - 1 + n_z * (2 * side * side - 1)
        n_acc = max(n_early, min(8, n_blocks))
        accs = [
            pltpu.ACC(q)((slots, TILE), jnp.float32)
            for _ in range(n_acc)
            for q in range(bc // TILE)
        ]
        vmem = pl.BlockSpec(memory_space=pltpu.VMEM)
        anywhere = pl.BlockSpec(memory_space=pl.ANY)
        gain_rows = gain.reshape(depth // LANES, LANES)
        packed = pl.pallas_call(
            functools.partial(kernel, n_v, n_b, n_early, accs),
            out_shape=jax.ShapeDtypeStruct((box, LANES), jnp.float32),
            in_specs=[anywhere] * 7,
            out_specs=vmem,
            scratch_shapes=[
                pltpu.VMEM((n_slots, kz, bc), jnp.bfloat16),
                pltpu.VMEM((n_v, n_b, group, fpd), jnp.bfloat16),
                pltpu.VMEM((n_z, slots, kz), jnp.bfloat16),
                pltpu.VMEM(gain_rows.shape, jnp.bfloat16),
                pltpu.VMEM(gain_rows.shape, jnp.float32),
                pltpu.VMEM((1, heat.shape[0]), jnp.float32),
                pltpu.VMEM((1, slots), jnp.int32),
                pltpu.VMEM(ids.shape, jnp.int32),
                pltpu.VMEM((1, slots), jnp.int32),
                pltpu.VMEM((n_z, 1, LANES), jnp.float32),
                pltpu.VMEM((n_p, 1, LANES), jnp.float32),
                pltpu.VMEM((2, 1, LANES), jnp.float32),
                pltpu.VMEM((n_b, box, LANES), jnp.float32),
                pltpu.VMEM((n_p, box, LANES), jnp.float32),
                pltpu.VMEM((box, LANES), jnp.float32),
                pltpu.VMEM((n_z, box, LANES), jnp.float32),
                pltpu.SemaphoreType.DMA((n_slots,)),
                pltpu.SemaphoreType.DMA((max(1, kz // LAST_ROWS),)),
                pltpu.SemaphoreType.DMA((6,)),
                pltpu.SemaphoreType.DMA((n_v, n_b)),
                pltpu.SemaphoreType.DMA((n_sends,)),
                pltpu.SemaphoreType.DMA((n_z,)),
                pltpu.SemaphoreType.DMA((n_z,)),
                pltpu.SemaphoreType.DMA((n_p,)),
                pltpu.SemaphoreType.DMA((n_p,)),
                pltpu.SemaphoreType.DMA((n_p,)),
                pltpu.SemaphoreType.DMA((n_p,)),
                pltpu.SemaphoreType.DMA((n_z,)),
                pltpu.SemaphoreType.DMA((n_z,)),
            ],
            compiler_params=pltpu.CompilerParams(
                collective_id=0,
                has_side_effects=True,
                vmem_limit_bytes=60 * 1024 * 1024,
            ),
        )(
            rows,
            gain_rows,
            w,
            heat.reshape(1, -1),
            choice.reshape(1, -1),
            ids,
            keep.reshape(1, -1),
        )
        log_norm, mass, renormed = pl.pallas_call(
            split,
            out_shape=(
                jax.ShapeDtypeStruct((1, group), jnp.float32),
                jax.ShapeDtypeStruct((1, group), jnp.float32),
                jax.ShapeDtypeStruct((group, ids.shape[1]), jnp.float32),
            ),
            in_specs=[vmem],
            out_specs=(vmem, vmem, vmem),
        )(packed)
        return log_norm.reshape(group), mass.reshape(group), renormed

    placed = (P("batch", "vocab"), P(), P(None, ("vocab", "batch")), P(), P(), P(), P())
    return jax.shard_map(
        local,
        mesh=mesh,
        in_specs=placed,
        out_specs=(P("batch"), P("batch"), P("batch", None)),
        check_vma=False,
    )
```

```python
import functools

import jax
import jax.numpy as jnp
from jax import lax
from jax.experimental import pallas as pl
from jax.experimental.pallas import tpu as pltpu
from jax.sharding import PartitionSpec as P

MESH = pl.DeviceIdType.MESH
epsilon = 1e-06
LANES = 128
TILE = 256
STAT_ROWS = 2
BLOCK_COLS = 512
STREAM_BYTES = 48 * 1024 * 1024
LAST_ROWS = 512
LOW = -3e38


def iota(shape, axis):
    return lax.broadcasted_iota(jnp.int32, shape, axis)


def column_to_row(column):
    rows = column.shape[0]
    diagonal = iota((rows, LANES), 0) == iota((rows, LANES), 1)
    return jnp.sum(jnp.where(diagonal, column, 0.0), axis=0, keepdims=True)


def row_to_column(row, first, rows):
    width = row.shape[1]
    diagonal = iota((rows, width), 0) + first == iota((rows, width), 1)
    return jnp.sum(jnp.where(diagonal, row, 0.0), axis=1, keepdims=True)


def combine(parts, group):
    candidates = parts[0][:group, :]
    top = parts[0][group : group + 1, :]
    for part in parts[1:]:
        candidates = candidates + part[:group, :]
        top = jnp.maximum(top, part[group : group + 1, :])
    total = jnp.zeros_like(top)
    for part in parts:
        total = total + part[group + 1 : group + 2, :] * jnp.exp(
            part[group : group + 1, :] - top
        )
    return candidates, top, total


def flip(value, j):
    out = value
    bit = 1
    while bit <= j:
        if j & bit:
            out = out + bit * (1 - 2 * ((value // bit) % 2))
        bit *= 2
    return out


def kernel(n_v, n_b, specs, *refs):
    pl.run_scoped(lambda *accs: program(n_v, n_b, accs, *refs), *specs)


def program(
    n_v,
    n_b,
    accs,
    x_hbm,
    gain_hbm,
    w_hbm,
    heat_hbm,
    choice_hbm,
    ids_hbm,
    keep_hbm,
    out_ref,
    wbuf,
    xbuf,
    lhs,
    gain_in,
    gain_row,
    heat_ref,
    choice_ref,
    ids_ref,
    keep_ref,
    z_stat,
    p_stat,
    stat_out,
    outbox,
    inbox,
    midbox,
    lastbox,
    w_sem,
    l_sem,
    in_sem,
    x_recv,
    x_send,
    z_recv,
    z_send,
    p_recv,
    p_send,
    t_recv,
    t_send,
    u_recv,
    u_send,
):
    v = lax.axis_index("vocab")
    b = lax.axis_index("batch")
    side = n_b // 2
    n_z = n_v // side
    z = v // side
    y = v % side
    x = b // 2
    c = b % 2
    n_p = 2 * side * side
    group, fpd = x_hbm.shape
    slots = n_b * group
    depth, cols = w_hbm.shape
    n_slots, kz, bc = wbuf.shape
    n_blocks = cols // bc
    halves = bc // TILE
    n_last = max(1, kz // LAST_ROWS)

    def device(x_, y_, z_, c_):
        return (z_ * side + y_, 2 * x_ + c_)

    def place(x_, y_, c_):
        return (x_ * side + y_) * 2 + c_

    mine = place(x, y, c)

    plane = []
    for dx in range(side):
        for dy in range(side):
            for dc in range(2):
                if dx + dy + dc > 0:
                    plane.append(((x + dx) % side, (y + dy) % side, (c + dc) % 2))
    order = [flip(z, j) for j in range(n_z)]

    barrier = pltpu.get_barrier_semaphore()
    for j in range(1, n_z):
        pl.semaphore_signal(
            barrier, inc=1, device_id=device(x, y, order[j], c), device_id_type=MESH
        )
    for px, py, pc in plane:
        pl.semaphore_signal(
            barrier, inc=1, device_id=device(px, py, z, pc), device_id_type=MESH
        )

    loads = [
        pltpu.make_async_copy(src, dst, in_sem.at[i])
        for i, (src, dst) in enumerate(
            [
                (x_hbm, xbuf.at[v, b]),
                (gain_hbm, gain_in),
                (heat_hbm, heat_ref),
                (choice_hbm, choice_ref),
                (ids_hbm, ids_ref),
                (keep_hbm, keep_ref),
            ]
        )
    ]
    for copy in loads:
        copy.start()

    tasks = [(j, n) for j in range(n_z) for n in range(n_blocks)]
    n_tasks = len(tasks)

    def stream(t):
        j, n = tasks[t]
        slot = t % n_slots
        row = pl.multiple_of(order[j] * kz, kz)
        columns = pl.ds(n * bc, bc)
        if t < n_tasks - 1:
            return [
                pltpu.make_async_copy(
                    w_hbm.at[pl.ds(row, kz), columns], wbuf.at[slot], w_sem.at[slot]
                )
            ]
        piece = kz // n_last
        return [
            pltpu.make_async_copy(
                w_hbm.at[pl.ds(row + i * piece, piece), columns],
                wbuf.at[slot, pl.ds(i * piece, piece)],
                l_sem.at[i],
            )
            for i in range(n_last)
        ]

    for t in range(min(n_slots, n_tasks)):
        for copy in stream(t):
            copy.start(priority=1)

    loads[0].wait()
    own = xbuf[v, b].astype(jnp.float32)
    own = own * own
    partial = own[:, :LANES]
    for t in range(1, fpd // LANES):
        partial = partial + own[:, t * LANES : (t + 1) * LANES]
    partial = column_to_row(jnp.sum(partial, axis=1, keepdims=True))
    stat_out[0] = partial
    z_stat[z] = partial

    pl.semaphore_wait(barrier, n_z - 1 + n_p - 1)

    sent = []

    def send(src, dst, send_sem, recv_sem, to):
        copy = pltpu.make_async_remote_copy(
            src_ref=src,
            dst_ref=dst,
            send_sem=send_sem,
            recv_sem=recv_sem,
            device_id=to,
            device_id_type=MESH,
        )
        copy.start()
        sent.append(copy)

    counter = [0]

    def forward(v_, b_, to):
        block = xbuf.at[v_, b_]
        send(block, block, x_send.at[counter[0]], x_recv.at[v_, b_], to)
        counter[0] += 1

    def arrived(v_, b_):
        pltpu.make_async_copy(x_hbm, xbuf.at[v_, b_], x_recv.at[v_, b_]).wait()

    same = [(dx, dy) for dx in range(side) for dy in range(side) if dx + dy > 0]
    same.sort(key=lambda d: d[1])

    for j in range(1, n_z):
        send(
            stat_out.at[0],
            z_stat.at[z],
            z_send.at[j],
            z_recv.at[z],
            device(x, y, order[j], c),
        )
    def step_z(j):
        v_ = order[j] * side + y
        if j > 0:
            arrived(v_, b)
        for dx, dy in same:
            forward(v_, b, device((x + dx) % side, (y + dy) % side, z, c))
        forward(v_, b, device(x, y, z, 1 - c))

    def step_p(j, dx, dy):
        px, py = (x - dx + side) % side, (y - dy + side) % side
        v_, b_ = order[j] * side + py, 2 * px + c
        arrived(v_, b_)
        forward(v_, b_, device(x, y, z, 1 - c))

    def stat_z():
        for j in range(1, n_z):
            source = order[j]
            pltpu.make_async_copy(
                stat_out.at[0], z_stat.at[source], z_recv.at[source]
            ).wait()
        total = z_stat[0]
        for j in range(1, n_z):
            total = total + z_stat[j]
        stat_out[1] = total
        p_stat[mine] = total
        for i, (px, py, pc) in enumerate(plane):
            send(
                stat_out.at[1],
                p_stat.at[mine],
                p_send.at[i],
                p_recv.at[mine],
                device(px, py, z, pc),
            )

    def stat_p():
        for px, py, pc in plane:
            source = place(px, py, pc)
            pltpu.make_async_copy(
                stat_out.at[1], p_stat.at[source], p_recv.at[source]
            ).wait()
        columns = []
        for bx in range(side):
            for bcore in range(2):
                total = p_stat[place(bx, 0, bcore)]
                for by in range(1, side):
                    total = total + p_stat[place(bx, by, bcore)]
                columns.append(row_to_column(total, 0, group))
        mean_square = jnp.concatenate(columns, axis=0) / depth
        return lax.rsqrt(mean_square + epsilon)

    step_z(0)
    for j in range(1, n_z):
        forward(v, b, device(x, y, order[j], c))

    for copy in loads[1:]:
        copy.wait()
    gain_row[...] = gain_in[...].astype(jnp.float32)
    level = [d for d in same if d[1] == 0]
    rest = [d for d in same if d[1] > 0]
    relays = [("p", 0, *d) for d in level] + [("z", 1)]
    relays += [("p", 0, *d) for d in rest]
    relays += [("z", j) for j in range(2, n_z - 1)] + [("stat",)]
    relays += [("z", n_z - 1)] if n_z > 2 else []
    relays += [("p", j, *d) for j in range(1, n_z) for d in same]
    steps = {"z": step_z, "p": step_p, "stat": stat_z}

    def relay(limit=n_z):
        if relays and (relays[0][0] != "p" or relays[0][1] <= limit):
            kind, *rest = relays.pop(0)
            steps[kind](*rest)

    def ensure(wanted):
        while any(wanted(item) for item in relays):
            relay()

    ensure(lambda item: item[0] == "p" and item[1] == 0 and item[3] == 0)
    ensure(lambda item: item == ("z", 1))

    choice = row_to_column(choice_ref[...].astype(jnp.float32), 0, slots)
    n_heat = heat_ref.shape[1]
    member = choice == iota((slots, n_heat), 1).astype(jnp.float32)
    heat = jnp.sum(jnp.where(member, heat_ref[...], 0.0), axis=1, keepdims=True)
    cool = 1.0 / heat

    local_ids = ids_ref[...] - (v * n_b + b) * cols
    tile_of = local_ids >> 7
    lane_of = local_ids & (LANES - 1)

    def feature_block(j, k):
        return order[j] * side + ((y + k) % side if j == 0 else k)

    def normalise(j, k, factor):
        at = feature_block(j, k)
        values = xbuf[at].reshape(slots, fpd).astype(jnp.float32)
        for t in range(fpd // LANES):
            part = values[:, t * LANES : (t + 1) * LANES]
            if factor is not None:
                part = part * factor
            gain = gain_row[pl.ds(at * (fpd // LANES) + t, 1), :]
            lhs[j, :, k * fpd + t * LANES : k * fpd + (t + 1) * LANES] = (
                part * gain
            ).astype(jnp.bfloat16)

    def partner_blocks(j, k):
        for bx in range(side):
            arrived(feature_block(j, k), 2 * bx + 1 - c)

    for acc in accs:
        pltpu.matmul_pop(acc)
    state = [
        jnp.full((slots, LANES), LOW, jnp.float32),
        jnp.zeros((slots, LANES), jnp.float32),
        jnp.zeros((slots, LANES), jnp.float32),
    ]

    def run(t, k=None):
        j, n = tasks[t]
        slot = t % n_slots
        pieces = stream(t)
        at = (2 * n + (j > 0)) * halves
        if k is None:
            rows = kz // len(pieces)
            spans = [(piece, i * rows, i * rows) for i, piece in enumerate(pieces)]
        else:
            rows = fpd
            if k == 0:
                for piece in pieces:
                    piece.wait()
            spans = [(None, k * fpd, ((y + k) % side) * fpd)]
        turn = 0
        for piece, left, row in spans:
            if piece is not None:
                piece.wait()
            for i in range(rows // TILE):
                r = left + i * TILE
                w = row + i * TILE
                if k is not None:
                    w = pl.multiple_of(w, TILE)
                for q in range(halves):
                    pltpu.matmul_push_rhs(
                        wbuf[slot, pl.ds(w, TILE), q * TILE : (q + 1) * TILE],
                        staging_register=turn % 2,
                        mxu_index=q,
                    )
                    pltpu.matmul_acc_lhs(
                        accs[at + q],
                        lhs[j, :, r : r + TILE],
                        load_staged_rhs=turn % 2,
                    )
                turn += 1
        if t + n_slots < n_tasks and k in (None, side - 1):
            for copy in stream(t + n_slots):
                copy.start(priority=1)

    def finish(n):
        top, total, picked = state
        at = 2 * n * halves
        parts = []
        for q in range(halves):
            scores = pltpu.matmul_pop(accs[at + q]) * warm
            scores = scores + pltpu.matmul_pop(accs[at + halves + q]) * cool
            for h in range(TILE // LANES):
                parts.append(scores[:, h * LANES : (h + 1) * LANES])
        new_top = top
        for i, part in enumerate(parts):
            new_top = jnp.maximum(new_top, part)
            found = jnp.take_along_axis(
                part, lane_of, axis=1, mode="promise_in_bounds"
            )
            picked = jnp.where(tile_of == n * (bc // LANES) + i, found, picked)
        total = total * jnp.exp(top - new_top)
        for part in parts:
            total = total + jnp.exp(part - new_top)
        state[:] = [new_top, total, picked]

    for k in range(side):
        if k > 0:
            ensure(lambda item: item[0] == "p" and item[1] == 0)
        partner_blocks(0, k)
        normalise(0, k, None)
        for n in range(n_blocks):
            run(n, k)
            late = k == side - 1 and n >= n_blocks - len(same)
            relay(1 if late else 0)
    ensure(lambda item: item[0] != "p")
    factor = stat_p()
    warm = factor * cool
    for j in range(1, n_z):
        ensure(lambda item: item[0] == "p" and item[1] == j)
        for k in range(side):
            partner_blocks(j, k)
            normalise(j, k, factor)
        for n in range(n_blocks):
            run(j * n_blocks + n)
            if j == n_z - 1 and n > 0:
                finish(n - 1)
            else:
                relay(j + 1 if n >= n_blocks // 2 - 1 else j)
    finish(n_blocks - 1)

    top, total, picked = state
    peak = jnp.max(top, axis=1, keepdims=True)
    total = jnp.sum(total * jnp.exp(top - peak), axis=1, keepdims=True)
    for p in range(n_b):
        rows = slice(p * group, (p + 1) * group)
        outbox[p, :group, :] = picked[rows, :]
        outbox[p, group : group + 1, :] = column_to_row(peak[rows, :])
        outbox[p, group + 1 : group + 2, :] = column_to_row(total[rows, :])

    for i, (px, py, pc) in enumerate(plane):
        send(
            outbox.at[2 * px + pc],
            inbox.at[mine],
            t_send.at[i],
            t_recv.at[mine],
            device(px, py, z, pc),
        )
    inbox[mine] = outbox[b]
    for px, py, pc in plane:
        source = place(px, py, pc)
        pltpu.make_async_copy(outbox.at[0], inbox.at[source], t_recv.at[source]).wait()
    candidates, top, total = combine([inbox[s] for s in range(n_p)], group)
    midbox[:group, :] = candidates
    midbox[group : group + 1, :] = top
    midbox[group + 1 : group + 2, :] = total
    for j in range(1, n_z):
        send(midbox, lastbox.at[z], u_send.at[j], u_recv.at[z], device(x, y, order[j], c))
    lastbox[z] = midbox[...]
    for j in range(1, n_z):
        source = order[j]
        pltpu.make_async_copy(midbox, lastbox.at[source], u_recv.at[source]).wait()
    candidates, top, total = combine([lastbox[s] for s in range(n_z)], group)

    log_norm = top + jnp.log(jnp.where(total > 0.0, total, 1.0))
    cutoff = row_to_column(keep_ref[...].astype(jnp.float32), b * group, group)
    kept = iota((group, LANES), 1).astype(jnp.float32) < cutoff
    kept_top = jnp.max(jnp.where(kept, candidates, LOW), axis=1, keepdims=True)
    shifted = jnp.where(kept, candidates - kept_top, 0.0)
    kept_exp = jnp.where(kept, jnp.exp(shifted), 0.0)
    kept_sum = jnp.sum(kept_exp, axis=1, keepdims=True)
    kept_log = column_to_row(kept_top + jnp.log(kept_sum))
    out_ref[:group, :] = kept_exp / kept_sum
    out_ref[group : group + 1, :] = log_norm
    out_ref[group + 1 : group + 2, :] = kept_log - log_norm
    for copy in sent:
        copy.wait_send()


def split(all_ref, norm_ref, mass_ref, renorm_ref):
    group = renorm_ref.shape[0]
    renorm_ref[...] = all_ref[:group, :]
    norm_ref[...] = all_ref[group : group + 1, :group]
    mass_ref[...] = all_ref[group + 1 : group + 2, :group]


def solution(mesh):
    n_v, n_b = mesh.shape["vocab"], mesh.shape["batch"]

    def local(rows, gain, w, heat, choice, ids, keep):
        group, fpd = rows.shape
        depth, cols = w.shape
        slots = n_b * group
        side = n_b // 2
        n_z = n_v // side
        n_p = 2 * side * side
        kz = depth // n_z
        bc = min(cols, BLOCK_COLS)
        n_blocks = cols // bc
        n_slots = min(n_z * n_blocks, max(2, STREAM_BYTES // (kz * bc * 2)))
        box = group + STAT_ROWS
        n_sends = n_z - 1 + n_z * (2 * side * side - 1)
        accs = [
            pltpu.ACC(q)((slots, TILE), jnp.float32)
            for _ in range(2 * n_blocks)
            for q in range(bc // TILE)
        ]
        vmem = pl.BlockSpec(memory_space=pltpu.VMEM)
        anywhere = pl.BlockSpec(memory_space=pl.ANY)
        gain_rows = gain.reshape(depth // LANES, LANES)
        packed = pl.pallas_call(
            functools.partial(kernel, n_v, n_b, accs),
            out_shape=jax.ShapeDtypeStruct((box, LANES), jnp.float32),
            in_specs=[anywhere] * 7,
            out_specs=vmem,
            scratch_shapes=[
                pltpu.VMEM((n_slots, kz, bc), jnp.bfloat16),
                pltpu.VMEM((n_v, n_b, group, fpd), jnp.bfloat16),
                pltpu.VMEM((n_z, slots, kz), jnp.bfloat16),
                pltpu.VMEM(gain_rows.shape, jnp.bfloat16),
                pltpu.VMEM(gain_rows.shape, jnp.float32),
                pltpu.VMEM((1, heat.shape[0]), jnp.float32),
                pltpu.VMEM((1, slots), jnp.int32),
                pltpu.VMEM(ids.shape, jnp.int32),
                pltpu.VMEM((1, slots), jnp.int32),
                pltpu.VMEM((n_z, 1, LANES), jnp.float32),
                pltpu.VMEM((n_p, 1, LANES), jnp.float32),
                pltpu.VMEM((2, 1, LANES), jnp.float32),
                pltpu.VMEM((n_b, box, LANES), jnp.float32),
                pltpu.VMEM((n_p, box, LANES), jnp.float32),
                pltpu.VMEM((box, LANES), jnp.float32),
                pltpu.VMEM((n_z, box, LANES), jnp.float32),
                pltpu.SemaphoreType.DMA((n_slots,)),
                pltpu.SemaphoreType.DMA((max(1, kz // LAST_ROWS),)),
                pltpu.SemaphoreType.DMA((6,)),
                pltpu.SemaphoreType.DMA((n_v, n_b)),
                pltpu.SemaphoreType.DMA((n_sends,)),
                pltpu.SemaphoreType.DMA((n_z,)),
                pltpu.SemaphoreType.DMA((n_z,)),
                pltpu.SemaphoreType.DMA((n_p,)),
                pltpu.SemaphoreType.DMA((n_p,)),
                pltpu.SemaphoreType.DMA((n_p,)),
                pltpu.SemaphoreType.DMA((n_p,)),
                pltpu.SemaphoreType.DMA((n_z,)),
                pltpu.SemaphoreType.DMA((n_z,)),
            ],
            compiler_params=pltpu.CompilerParams(
                collective_id=0,
                has_side_effects=True,
                vmem_limit_bytes=60 * 1024 * 1024,
            ),
        )(
            rows,
            gain_rows,
            w,
            heat.reshape(1, -1),
            choice.reshape(1, -1),
            ids,
            keep.reshape(1, -1),
        )
        log_norm, mass, renormed = pl.pallas_call(
            split,
            out_shape=(
                jax.ShapeDtypeStruct((1, group), jnp.float32),
                jax.ShapeDtypeStruct((1, group), jnp.float32),
                jax.ShapeDtypeStruct((group, ids.shape[1]), jnp.float32),
            ),
            in_specs=[vmem],
            out_specs=(vmem, vmem, vmem),
        )(packed)
        return log_norm.reshape(group), mass.reshape(group), renormed

    placed = (P("batch", "vocab"), P(), P(None, ("vocab", "batch")), P(), P(), P(), P())
    return jax.shard_map(
        local,
        mesh=mesh,
        in_specs=placed,
        out_specs=(P("batch"), P("batch"), P("batch", None)),
        check_vma=False,
    )
```

```python
import functools

import jax
import jax.numpy as jnp
from jax import lax
from jax.experimental import pallas as pl
from jax.experimental.pallas import tpu as pltpu
from jax.sharding import PartitionSpec as P

MESH = pl.DeviceIdType.MESH
epsilon = 1e-06
LANES = 128
TILE = 256
STAT_ROWS = 2
BLOCK_COLS = 512
STREAM_BYTES = 48 * 1024 * 1024
LAST_ROWS = 512
LOW = -3e38


def iota(shape, axis):
    return lax.broadcasted_iota(jnp.int32, shape, axis)


def column_to_row(column):
    rows = column.shape[0]
    diagonal = iota((rows, LANES), 0) == iota((rows, LANES), 1)
    return jnp.sum(jnp.where(diagonal, column, 0.0), axis=0, keepdims=True)


def row_to_column(row, first, rows):
    width = row.shape[1]
    diagonal = iota((rows, width), 0) + first == iota((rows, width), 1)
    return jnp.sum(jnp.where(diagonal, row, 0.0), axis=1, keepdims=True)


def combine(parts, group):
    candidates = parts[0][:group, :]
    top = parts[0][group : group + 1, :]
    for part in parts[1:]:
        candidates = candidates + part[:group, :]
        top = jnp.maximum(top, part[group : group + 1, :])
    total = jnp.zeros_like(top)
    for part in parts:
        total = total + part[group + 1 : group + 2, :] * jnp.exp(
            part[group : group + 1, :] - top
        )
    return candidates, top, total


def flip(value, j):
    out = value
    bit = 1
    while bit <= j:
        if j & bit:
            out = out + bit * (1 - 2 * ((value // bit) % 2))
        bit *= 2
    return out


def kernel(n_v, n_b, specs, *refs):
    pl.run_scoped(lambda *accs: program(n_v, n_b, accs, *refs), *specs)


def program(
    n_v,
    n_b,
    accs,
    x_hbm,
    gain_hbm,
    w_hbm,
    heat_hbm,
    choice_hbm,
    ids_hbm,
    keep_hbm,
    out_ref,
    wbuf,
    xbuf,
    lhs,
    gain_in,
    gain_row,
    heat_ref,
    choice_ref,
    ids_ref,
    keep_ref,
    z_stat,
    p_stat,
    stat_out,
    outbox,
    inbox,
    midbox,
    lastbox,
    w_sem,
    l_sem,
    in_sem,
    x_recv,
    x_send,
    z_recv,
    z_send,
    p_recv,
    p_send,
    t_recv,
    t_send,
    u_recv,
    u_send,
):
    v = lax.axis_index("vocab")
    b = lax.axis_index("batch")
    side = n_b // 2
    n_z = n_v // side
    z = v // side
    y = v % side
    x = b // 2
    c = b % 2
    n_p = 2 * side * side
    group, fpd = x_hbm.shape
    slots = n_b * group
    depth, cols = w_hbm.shape
    n_slots, kz, bc = wbuf.shape
    n_blocks = cols // bc
    halves = bc // TILE
    n_last = max(1, kz // LAST_ROWS)

    def device(x_, y_, z_, c_):
        return (z_ * side + y_, 2 * x_ + c_)

    def place(x_, y_, c_):
        return (x_ * side + y_) * 2 + c_

    mine = place(x, y, c)

    steps = [(dx, dy, dc) for dx in range(side) for dy in range(side) for dc in range(2)]
    steps.sort(key=lambda d: -2 * ((d[0] > 0) + (d[1] > 0)) - d[2])
    plane = [
        ((x + dx) % side, (y + dy) % side, (c + dc) % 2)
        for dx, dy, dc in steps
        if dx + dy + dc > 0
    ]
    order = [flip(z, j) for j in range(n_z)]

    barrier = pltpu.get_barrier_semaphore()
    for j in reversed(range(1, n_z)):
        pl.semaphore_signal(
            barrier, inc=1, device_id=device(x, y, order[j], c), device_id_type=MESH
        )
    for px, py, pc in plane:
        pl.semaphore_signal(
            barrier, inc=1, device_id=device(px, py, z, pc), device_id_type=MESH
        )

    loads = [
        pltpu.make_async_copy(src, dst, in_sem.at[i])
        for i, (src, dst) in enumerate(
            [
                (x_hbm, xbuf.at[v, b]),
                (gain_hbm, gain_in),
                (heat_hbm, heat_ref),
                (choice_hbm, choice_ref),
                (ids_hbm, ids_ref),
                (keep_hbm, keep_ref),
            ]
        )
    ]
    for copy in loads:
        copy.start()

    tasks = [(j, n) for j in range(n_z) for n in range(n_blocks)]
    n_tasks = len(tasks)

    def stream(t):
        j, n = tasks[t]
        slot = t % n_slots
        row = pl.multiple_of(order[j] * kz, kz)
        columns = pl.ds(n * bc, bc)
        if t < n_tasks - 1:
            return [
                pltpu.make_async_copy(
                    w_hbm.at[pl.ds(row, kz), columns], wbuf.at[slot], w_sem.at[slot]
                )
            ]
        piece = kz // n_last
        return [
            pltpu.make_async_copy(
                w_hbm.at[pl.ds(row + i * piece, piece), columns],
                wbuf.at[slot, pl.ds(i * piece, piece)],
                l_sem.at[i],
            )
            for i in range(n_last)
        ]

    for t in range(min(n_slots, n_tasks)):
        for copy in stream(t):
            copy.start(priority=1)

    loads[0].wait()
    own = xbuf[v, b].astype(jnp.float32)
    own = own * own
    partial = own[:, :LANES]
    for t in range(1, fpd // LANES):
        partial = partial + own[:, t * LANES : (t + 1) * LANES]
    partial = column_to_row(jnp.sum(partial, axis=1, keepdims=True))
    stat_out[0] = partial
    z_stat[z] = partial

    pl.semaphore_wait(barrier, n_z - 1 + n_p - 1)

    sent = []

    def send(src, dst, send_sem, recv_sem, to):
        copy = pltpu.make_async_remote_copy(
            src_ref=src,
            dst_ref=dst,
            send_sem=send_sem,
            recv_sem=recv_sem,
            device_id=to,
            device_id_type=MESH,
        )
        copy.start()
        sent.append(copy)

    counter = [0]

    def forward(v_, b_, to):
        block = xbuf.at[v_, b_]
        send(block, block, x_send.at[counter[0]], x_recv.at[v_, b_], to)
        counter[0] += 1

    def arrived(v_, b_):
        pltpu.make_async_copy(x_hbm, xbuf.at[v_, b_], x_recv.at[v_, b_]).wait()

    same = [(dx, dy) for dx in range(side) for dy in range(side) if dx + dy > 0]
    same.sort(key=lambda d: d[1])

    for j in reversed(range(1, n_z)):
        send(
            stat_out.at[0],
            z_stat.at[z],
            z_send.at[j],
            z_recv.at[z],
            device(x, y, order[j], c),
        )
    def step_z(j):
        v_ = order[j] * side + y
        if j > 0:
            arrived(v_, b)
        for dx, dy in same:
            forward(v_, b, device((x + dx) % side, (y + dy) % side, z, c))
        forward(v_, b, device(x, y, z, 1 - c))

    def step_p(j, dx, dy):
        px, py = (x - dx + side) % side, (y - dy + side) % side
        v_, b_ = order[j] * side + py, 2 * px + c
        arrived(v_, b_)
        forward(v_, b_, device(x, y, z, 1 - c))

    def stat_z():
        for j in range(1, n_z):
            source = order[j]
            pltpu.make_async_copy(
                stat_out.at[0], z_stat.at[source], z_recv.at[source]
            ).wait()
        total = z_stat[0]
        for j in range(1, n_z):
            total = total + z_stat[j]
        stat_out[1] = total
        p_stat[mine] = total
        for i, (px, py, pc) in enumerate(plane):
            send(
                stat_out.at[1],
                p_stat.at[mine],
                p_send.at[i],
                p_recv.at[mine],
                device(px, py, z, pc),
            )

    def stat_p():
        for px, py, pc in plane:
            source = place(px, py, pc)
            pltpu.make_async_copy(
                stat_out.at[1], p_stat.at[source], p_recv.at[source]
            ).wait()
        columns = []
        for bx in range(side):
            for bcore in range(2):
                total = p_stat[place(bx, 0, bcore)]
                for by in range(1, side):
                    total = total + p_stat[place(bx, by, bcore)]
                columns.append(row_to_column(total, 0, group))
        mean_square = jnp.concatenate(columns, axis=0) / depth
        return lax.rsqrt(mean_square + epsilon)

    step_z(0)
    for j in range(1, n_z):
        forward(v, b, device(x, y, order[j], c))

    for copy in loads[1:]:
        copy.wait()
    gain_row[...] = gain_in[...].astype(jnp.float32)
    level = [d for d in same if d[1] == 0]
    rest = [d for d in same if d[1] > 0]
    relays = [("p", 0, *d) for d in level] + [("z", 1)]
    relays += [("p", 0, *d) for d in rest]
    relays += [("z", j) for j in range(2, n_z - 1)] + [("stat",)]
    relays += [("z", n_z - 1)] if n_z > 2 else []
    relays += [("p", j, *d) for j in range(1, n_z) for d in same]
    steps = {"z": step_z, "p": step_p, "stat": stat_z}

    def relay(limit=n_z):
        if relays and (relays[0][0] != "p" or relays[0][1] <= limit):
            kind, *rest = relays.pop(0)
            steps[kind](*rest)

    def ensure(wanted):
        while any(wanted(item) for item in relays):
            relay()

    ensure(lambda item: item[0] == "p" and item[1] == 0 and item[3] == 0)
    ensure(lambda item: item == ("z", 1))

    choice = row_to_column(choice_ref[...].astype(jnp.float32), 0, slots)
    n_heat = heat_ref.shape[1]
    member = choice == iota((slots, n_heat), 1).astype(jnp.float32)
    heat = jnp.sum(jnp.where(member, heat_ref[...], 0.0), axis=1, keepdims=True)
    cool = 1.0 / heat

    local_ids = ids_ref[...] - (v * n_b + b) * cols
    tile_of = local_ids >> 7
    lane_of = local_ids & (LANES - 1)

    def feature_block(j, k):
        return order[j] * side + ((y + k) % side if j == 0 else k)

    def normalise(j, k, factor):
        at = feature_block(j, k)
        values = xbuf[at].reshape(slots, fpd).astype(jnp.float32)
        for t in range(fpd // LANES):
            part = values[:, t * LANES : (t + 1) * LANES]
            if factor is not None:
                part = part * factor
            gain = gain_row[pl.ds(at * (fpd // LANES) + t, 1), :]
            lhs[j, :, k * fpd + t * LANES : k * fpd + (t + 1) * LANES] = (
                part * gain
            ).astype(jnp.bfloat16)

    def partner_blocks(j, k):
        for bx in range(side):
            arrived(feature_block(j, k), 2 * bx + 1 - c)

    for acc in accs:
        pltpu.matmul_pop(acc)
    state = [
        jnp.full((slots, LANES), LOW, jnp.float32),
        jnp.zeros((slots, LANES), jnp.float32),
        jnp.zeros((slots, LANES), jnp.float32),
    ]

    def run(t, k=None):
        j, n = tasks[t]
        slot = t % n_slots
        pieces = stream(t)
        at = (2 * n + (j > 0)) * halves
        if k is None:
            rows = kz // len(pieces)
            spans = [(piece, i * rows, i * rows) for i, piece in enumerate(pieces)]
        else:
            rows = fpd
            if k == 0:
                for piece in pieces:
                    piece.wait()
            spans = [(None, k * fpd, ((y + k) % side) * fpd)]
        turn = 0
        for piece, left, row in spans:
            if piece is not None:
                piece.wait()
            for i in range(rows // TILE):
                r = left + i * TILE
                w = row + i * TILE
                if k is not None:
                    w = pl.multiple_of(w, TILE)
                for q in range(halves):
                    pltpu.matmul_push_rhs(
                        wbuf[slot, pl.ds(w, TILE), q * TILE : (q + 1) * TILE],
                        staging_register=turn % 2,
                        mxu_index=q,
                    )
                    pltpu.matmul_acc_lhs(
                        accs[at + q],
                        lhs[j, :, r : r + TILE],
                        load_staged_rhs=turn % 2,
                    )
                turn += 1
        if t + n_slots < n_tasks and k in (None, side - 1):
            for copy in stream(t + n_slots):
                copy.start(priority=1)

    def finish(n):
        top, total, picked = state
        at = 2 * n * halves
        parts = []
        for q in range(halves):
            scores = pltpu.matmul_pop(accs[at + q]) * warm
            scores = scores + pltpu.matmul_pop(accs[at + halves + q]) * cool
            for h in range(TILE // LANES):
                parts.append(scores[:, h * LANES : (h + 1) * LANES])
        new_top = top
        for i, part in enumerate(parts):
            new_top = jnp.maximum(new_top, part)
            found = jnp.take_along_axis(
                part, lane_of, axis=1, mode="promise_in_bounds"
            )
            picked = jnp.where(tile_of == n * (bc // LANES) + i, found, picked)
        total = total * jnp.exp(top - new_top)
        for part in parts:
            total = total + jnp.exp(part - new_top)
        state[:] = [new_top, total, picked]

    for k in range(side):
        if k > 0:
            ensure(lambda item: item[0] == "p" and item[1] == 0)
        partner_blocks(0, k)
        normalise(0, k, None)
        for n in range(n_blocks):
            run(n, k)
            late = k == side - 1 and n >= n_blocks - len(same)
            relay(1 if late else 0)
    ensure(lambda item: item[0] != "p")
    factor = stat_p()
    warm = factor * cool
    for j in range(1, n_z):
        ensure(lambda item: item[0] == "p" and item[1] == j)
        for k in range(side):
            partner_blocks(j, k)
            normalise(j, k, factor)
        for n in range(n_blocks):
            run(j * n_blocks + n)
            if j == n_z - 1 and n > 0:
                finish(n - 1)
            else:
                relay(j + 1 if n >= n_blocks // 2 - 1 else j)
    finish(n_blocks - 1)

    top, total, picked = state
    peak = jnp.max(top, axis=1, keepdims=True)
    total = jnp.sum(total * jnp.exp(top - peak), axis=1, keepdims=True)
    for p in range(n_b):
        rows = slice(p * group, (p + 1) * group)
        outbox[p, :group, :] = picked[rows, :]
        outbox[p, group : group + 1, :] = column_to_row(peak[rows, :])
        outbox[p, group + 1 : group + 2, :] = column_to_row(total[rows, :])

    for i, (px, py, pc) in enumerate(plane):
        send(
            outbox.at[2 * px + pc],
            inbox.at[mine],
            t_send.at[i],
            t_recv.at[mine],
            device(px, py, z, pc),
        )
    inbox[mine] = outbox[b]
    for px, py, pc in plane:
        source = place(px, py, pc)
        pltpu.make_async_copy(outbox.at[0], inbox.at[source], t_recv.at[source]).wait()
    candidates, top, total = combine([inbox[s] for s in range(n_p)], group)
    midbox[:group, :] = candidates
    midbox[group : group + 1, :] = top
    midbox[group + 1 : group + 2, :] = total
    for j in reversed(range(1, n_z)):
        send(midbox, lastbox.at[z], u_send.at[j], u_recv.at[z], device(x, y, order[j], c))
    lastbox[z] = midbox[...]
    for j in range(1, n_z):
        source = order[j]
        pltpu.make_async_copy(midbox, lastbox.at[source], u_recv.at[source]).wait()
    candidates, top, total = combine([lastbox[s] for s in range(n_z)], group)

    log_norm = top + jnp.log(jnp.where(total > 0.0, total, 1.0))
    cutoff = row_to_column(keep_ref[...].astype(jnp.float32), b * group, group)
    kept = iota((group, LANES), 1).astype(jnp.float32) < cutoff
    kept_top = jnp.max(jnp.where(kept, candidates, LOW), axis=1, keepdims=True)
    shifted = jnp.where(kept, candidates - kept_top, 0.0)
    kept_exp = jnp.where(kept, jnp.exp(shifted), 0.0)
    kept_sum = jnp.sum(kept_exp, axis=1, keepdims=True)
    kept_log = column_to_row(kept_top + jnp.log(kept_sum))
    out_ref[:group, :] = kept_exp / kept_sum
    out_ref[group : group + 1, :] = log_norm
    out_ref[group + 1 : group + 2, :] = kept_log - log_norm
    for copy in sent:
        copy.wait_send()


def split(all_ref, norm_ref, mass_ref, renorm_ref):
    group = renorm_ref.shape[0]
    renorm_ref[...] = all_ref[:group, :]
    norm_ref[...] = all_ref[group : group + 1, :group]
    mass_ref[...] = all_ref[group + 1 : group + 2, :group]


def solution(mesh):
    n_v, n_b = mesh.shape["vocab"], mesh.shape["batch"]

    def local(rows, gain, w, heat, choice, ids, keep):
        group, fpd = rows.shape
        depth, cols = w.shape
        slots = n_b * group
        side = n_b // 2
        n_z = n_v // side
        n_p = 2 * side * side
        kz = depth // n_z
        bc = min(cols, BLOCK_COLS)
        n_blocks = cols // bc
        n_slots = min(n_z * n_blocks, max(2, STREAM_BYTES // (kz * bc * 2)))
        box = group + STAT_ROWS
        n_sends = n_z - 1 + n_z * (2 * side * side - 1)
        accs = [
            pltpu.ACC(q)((slots, TILE), jnp.float32)
            for _ in range(2 * n_blocks)
            for q in range(bc // TILE)
        ]
        vmem = pl.BlockSpec(memory_space=pltpu.VMEM)
        anywhere = pl.BlockSpec(memory_space=pl.ANY)
        gain_rows = gain.reshape(depth // LANES, LANES)
        packed = pl.pallas_call(
            functools.partial(kernel, n_v, n_b, accs),
            out_shape=jax.ShapeDtypeStruct((box, LANES), jnp.float32),
            in_specs=[anywhere] * 7,
            out_specs=vmem,
            scratch_shapes=[
                pltpu.VMEM((n_slots, kz, bc), jnp.bfloat16),
                pltpu.VMEM((n_v, n_b, group, fpd), jnp.bfloat16),
                pltpu.VMEM((n_z, slots, kz), jnp.bfloat16),
                pltpu.VMEM(gain_rows.shape, jnp.bfloat16),
                pltpu.VMEM(gain_rows.shape, jnp.float32),
                pltpu.VMEM((1, heat.shape[0]), jnp.float32),
                pltpu.VMEM((1, slots), jnp.int32),
                pltpu.VMEM(ids.shape, jnp.int32),
                pltpu.VMEM((1, slots), jnp.int32),
                pltpu.VMEM((n_z, 1, LANES), jnp.float32),
                pltpu.VMEM((n_p, 1, LANES), jnp.float32),
                pltpu.VMEM((2, 1, LANES), jnp.float32),
                pltpu.VMEM((n_b, box, LANES), jnp.float32),
                pltpu.VMEM((n_p, box, LANES), jnp.float32),
                pltpu.VMEM((box, LANES), jnp.float32),
                pltpu.VMEM((n_z, box, LANES), jnp.float32),
                pltpu.SemaphoreType.DMA((n_slots,)),
                pltpu.SemaphoreType.DMA((max(1, kz // LAST_ROWS),)),
                pltpu.SemaphoreType.DMA((6,)),
                pltpu.SemaphoreType.DMA((n_v, n_b)),
                pltpu.SemaphoreType.DMA((n_sends,)),
                pltpu.SemaphoreType.DMA((n_z,)),
                pltpu.SemaphoreType.DMA((n_z,)),
                pltpu.SemaphoreType.DMA((n_p,)),
                pltpu.SemaphoreType.DMA((n_p,)),
                pltpu.SemaphoreType.DMA((n_p,)),
                pltpu.SemaphoreType.DMA((n_p,)),
                pltpu.SemaphoreType.DMA((n_z,)),
                pltpu.SemaphoreType.DMA((n_z,)),
            ],
            compiler_params=pltpu.CompilerParams(
                collective_id=0,
                has_side_effects=True,
                vmem_limit_bytes=60 * 1024 * 1024,
            ),
        )(
            rows,
            gain_rows,
            w,
            heat.reshape(1, -1),
            choice.reshape(1, -1),
            ids,
            keep.reshape(1, -1),
        )
        log_norm, mass, renormed = pl.pallas_call(
            split,
            out_shape=(
                jax.ShapeDtypeStruct((1, group), jnp.float32),
                jax.ShapeDtypeStruct((1, group), jnp.float32),
                jax.ShapeDtypeStruct((group, ids.shape[1]), jnp.float32),
            ),
            in_specs=[vmem],
            out_specs=(vmem, vmem, vmem),
        )(packed)
        return log_norm.reshape(group), mass.reshape(group), renormed

    placed = (P("batch", "vocab"), P(), P(None, ("vocab", "batch")), P(), P(), P(), P())
    return jax.shard_map(
        local,
        mesh=mesh,
        in_specs=placed,
        out_specs=(P("batch"), P("batch"), P("batch", None)),
        check_vma=False,
    )
```
